32 devices in a mesh: patch: 16 (over z, y, x), pair: 2 (over core).
Axes of the slice: x: 2, y: 2, z: 4, core: 2. Of those that a mesh axis runs over, the one named last changes fastest.
Arguments:
- node_latent: bfloat16 [5120, 512], P('patch'), may hold values from -6 to 6
- edge_latent: bfloat16 [65536, 512], P(('patch', 'pair')), may hold values from -6 to 6
- edge_sender: int32 [65536], P(('patch', 'pair')), may hold values from 0 to 255
- edge_receiver: int32 [65536], P(('patch', 'pair')), may hold values from 0 to 319
- edge_count: int32 [32], P(('patch', 'pair')), may hold values from 1 to 2048, 32768 in all
- send_rows: int32 [16, 16, 16], P('patch'), may hold values from 0 to 319
- w_edge: bfloat16 [512, 512], replicated, may hold values from -0.15625 to 0.15625
- w_send: bfloat16 [512, 512], replicated, may hold values from -0.15625 to 0.15625
- w_recv: bfloat16 [512, 512], replicated, may hold values from -0.15625 to 0.15625
- edge_bias: float32 [512], replicated, may hold values from -4 to 4
- edge_out: bfloat16 [512, 512], replicated, may hold values from -0.25 to 0.25
- edge_out_bias: float32 [512], replicated, may hold values from -4 to 4
- edge_gain: float32 [512], replicated, may hold values from 0.25 to 1.75
- edge_offset: float32 [512], replicated, may hold values from -2 to 2
- w_node: bfloat16 [512, 512], replicated, may hold values from -0.1875 to 0.1875
- w_agg: bfloat16 [512, 512], replicated, may hold values from -0.1875 to 0.1875
- node_bias: float32 [512], replicated, may hold values from -4 to 4
- node_out: bfloat16 [512, 512], replicated, may hold values from -0.25 to 0.25
- node_out_bias: float32 [512], replicated, may hold values from -4 to 4
- node_gain: float32 [512], replicated, may hold values from 0.25 to 1.75
- node_offset: float32 [512], replicated, may hold values from -2 to 2
Outputs:
- new_edge: bfloat16 [65536, 512], P(('patch', 'pair'))
- new_node: bfloat16 [5120, 512], P('patch')
The draws below stay inside these ranges and needn't reach their ends.
Inputs may be any that keep to these rules, and one draw needn't show every extreme that they name: `edge_count`: the valid edges of a device are the first ones of its block; some device's block is full.
All inputs are finite; a program needn't handle non-finite values.
Results may differ from the reference program's by a relative error of at most 0.007.
Values may be sent and summed in bfloat16 or wider, within the bound.
A program may use at most 64 MiB of HBM per device.

```python
import math
import jax
import jax.numpy as jnp
import numpy as np
from jax import lax

D = 512
NODE_DEV = 320
EDGE_DEV = 2048
SLOT = 16
NODES = 5120
EDGES = 65536
N_PATCH = 16
N_PAIR = 2


def plant(entries, rng, low, top_value):
    index_at = [jax.random.randint(jax.random.fold_in(rng, axis), (), 0, length) for axis, length in enumerate(entries.shape)]
    main_axis = entries.shape.index(max(entries.shape))
    neighbour = index_at[:main_axis] + [(index_at[main_axis] + 1) % entries.shape[main_axis]] + index_at[main_axis + 1:]
    return entries.at[tuple(index_at)].set(low).at[tuple(neighbour)].set(top_value)


def shard_levels(rng, shape, split, smallest, high):
    level = 1.0
    for position, shards_of in split:
        draws = jax.random.uniform(jax.random.fold_in(jax.random.fold_in(rng, 6), position), (shards_of,), jnp.float32, smallest / len(split), high / len(split))
        level = level * jnp.repeat(jnp.exp(draws), shape[position] // shards_of).reshape((-1,) + (1,) * (len(shape) - 1 - position))
    return level


def length_profile(number_of, total, reach, slope):
    loads = [(1 << 20) // math.isqrt(rank ** slope) + 1 for rank in range(2, number_of + 1)]
    spare, holding = total - reach - (number_of - 1), [1] * (number_of - 1)
    while spare > 0:
        movable = [i for i in range(number_of - 1) if holding[i] < reach]
        mass, budget = sum([loads[i] for i in movable]), spare
        for i in movable:
            more = min(reach - holding[i], max(1, budget * loads[i] // mass), spare)
            holding[i] = holding[i] + more
            spare = spare - more
    return np.array([reach] + holding)


def uneven(own_key, amount, total, reach, skew):
    if amount == 2:
        one = jax.random.randint(own_key, (), max(1, total - reach), min(reach, total - 1) + 1)
        return jnp.stack([one, total - one])
    lengths = jnp.asarray(length_profile(amount, total, reach, skew), jnp.int32)
    twos = (amount - 1) // 2
    source_of, taker = lengths[1:1 + 2 * twos:2], lengths[2:2 + 2 * twos:2]
    room = jnp.minimum(source_of - 1, reach - taker)
    passed = jax.random.randint(jax.random.fold_in(own_key, 1), (twos,), 0, 1 << 20) % (room + 1)
    lengths = lengths.at[1:1 + 2 * twos:2].set(source_of - passed).at[2:2 + 2 * twos:2].set(taker + passed)
    return lengths[jax.random.permutation(jax.random.fold_in(own_key, 2), amount)]


def normal_values(stream_key, dims, deviation, most, shards=(), kind=jnp.bfloat16):
    loudness = shard_levels(stream_key, dims, shards, -0.22, 0.18) if shards else 1.0
    entries = jax.random.normal(stream_key, dims, jnp.float32) * deviation * loudness
    return jnp.minimum(jnp.maximum(entries, -most), most).astype(kind)


def setup_inputs(seed: int = 0) -> dict:
    splits = jax.random.split(jax.random.key(seed), 22)
    node_latent = normal_values(splits[0], (NODES, D), 1.0, 6.0, ((0, 16),))
    edge_latent = normal_values(splits[1], (EDGES, D), 1.0, 6.0, ((0, 32),))
    edge_sender = plant(jax.random.randint(splits[2], (EDGES,), 0, N_PATCH * SLOT), jax.random.fold_in(splits[2], 1), 0, (N_PATCH * SLOT) - 1).astype(jnp.int32)
    edge_receiver = plant(jax.random.randint(splits[3], (EDGES,), 0, NODE_DEV), jax.random.fold_in(splits[3], 1), 0, NODE_DEV - 1).astype(jnp.int32)
    edge_count = uneven(splits[4], N_PATCH * N_PAIR, EDGE_DEV * N_PATCH, EDGE_DEV, 2).astype(jnp.int32)
    send_rows = plant(jax.random.randint(splits[5], (N_PATCH, N_PATCH, SLOT), 0, NODE_DEV), jax.random.fold_in(splits[5], 1), 0, NODE_DEV - 1).astype(jnp.int32)
    w_edge = normal_values(splits[6], (D, D), (3 * D) ** -0.5, 0.15625)
    w_send = normal_values(splits[7], (D, D), (3 * D) ** -0.5, 0.15625)
    w_recv = normal_values(splits[8], (D, D), (3 * D) ** -0.5, 0.15625)
    edge_bias = normal_values(splits[9], (D,), 1.0, 4.0, (), jnp.float32)
    edge_out = normal_values(splits[10], (D, D), D ** -0.5, 0.25)
    edge_out_bias = normal_values(splits[11], (D,), 1.0, 4.0, (), jnp.float32)
    edge_gain = jnp.clip(1.0 + 0.15 * jax.random.normal(splits[12], (D,), jnp.float32), 0.25, 1.75)
    edge_offset = normal_values(splits[13], (D,), 0.3, 2.0, (), jnp.float32)
    w_node = normal_values(splits[14], (D, D), (2 * D) ** -0.5, 0.1875)
    w_agg = normal_values(splits[15], (D, D), (2 * D) ** -0.5, 0.1875)
    node_bias = normal_values(splits[16], (D,), 1.0, 4.0, (), jnp.float32)
    node_out = normal_values(splits[17], (D, D), D ** -0.5, 0.25)
    node_out_bias = normal_values(splits[18], (D,), 1.0, 4.0, (), jnp.float32)
    node_gain = jnp.clip(1.0 + 0.15 * jax.random.normal(splits[19], (D,), jnp.float32), 0.25, 1.75)
    node_offset = normal_values(splits[20], (D,), 0.3, 2.0, (), jnp.float32)
    return dict(node_latent=node_latent, edge_latent=edge_latent, edge_sender=edge_sender, edge_receiver=edge_receiver, edge_count=edge_count, send_rows=send_rows, w_edge=w_edge, w_send=w_send, w_recv=w_recv, edge_bias=edge_bias, edge_out=edge_out, edge_out_bias=edge_out_bias, edge_gain=edge_gain, edge_offset=edge_offset, w_node=w_node, w_agg=w_agg, node_bias=node_bias, node_out=node_out, node_out_bias=node_out_bias, node_gain=node_gain, node_offset=node_offset)


def layer_norm(values, gain, offset):
    mean = lax.optimization_barrier(jnp.mean(values, axis=-1, keepdims=True))
    centered = values - mean
    spread = lax.optimization_barrier(jnp.mean(centered * centered, axis=-1, keepdims=True))
    return centered * lax.rsqrt(spread + 1e-05) * gain + offset

def reference(node_latent, edge_latent, edge_sender, edge_receiver, edge_count, send_rows, w_edge, w_send, w_recv, edge_bias, edge_out, edge_out_bias, edge_gain, edge_offset, w_node, w_agg, node_bias, node_out, node_out_bias, node_gain, node_offset):
    blocks = N_PATCH * N_PAIR
    proj_send = jnp.dot(node_latent, w_send, preferred_element_type=jnp.float32).astype(jnp.bfloat16)
    proj_recv = jnp.dot(node_latent, w_recv, preferred_element_type=jnp.float32)
    edge_blocks = edge_latent.reshape(blocks, EDGE_DEV, D)
    sender_blocks = edge_sender.reshape(blocks, EDGE_DEV)
    receiver_blocks = edge_receiver.reshape(blocks, EDGE_DEV)
    node_ids = jnp.arange(NODE_DEV, dtype=jnp.int32)

    def one_block(items):
        block, edges, senders, receivers, count = items
        patch = block // N_PAIR
        source = senders // SLOT
        within = senders % SLOT
        global_send = source * NODE_DEV + send_rows[source, patch, within]
        global_recv = patch * NODE_DEV + receivers
        pre = jnp.dot(edges, w_edge, preferred_element_type=jnp.float32) + proj_send[global_send].astype(jnp.float32) + proj_recv[global_recv] + edge_bias
        hidden = jax.nn.silu(pre).astype(jnp.bfloat16)
        message = jnp.dot(hidden, edge_out, preferred_element_type=jnp.float32) + edge_out_bias
        delta = layer_norm(message, edge_gain, edge_offset).astype(jnp.bfloat16)
        valid = jnp.arange(EDGE_DEV, dtype=jnp.int32) < count
        updated = (edges.astype(jnp.float32) + delta.astype(jnp.float32)).astype(jnp.bfloat16)
        updated = jnp.where(valid[:, None], updated, edges)
        onehot = ((receivers[None, :] == node_ids[:, None]) & valid[None, :]).astype(jnp.bfloat16)
        partial_value = jnp.dot(onehot, delta, preferred_element_type=jnp.float32)
        return (updated, partial_value)
    new_blocks, partials = lax.map(one_block, (jnp.arange(blocks, dtype=jnp.int32), edge_blocks, sender_blocks, receiver_blocks, edge_count))
    new_edge = new_blocks.reshape(EDGES, D)
    aggregate = lax.optimization_barrier(jnp.sum(partials.reshape(N_PATCH, N_PAIR, NODE_DEV, D), axis=1)).reshape(NODES, D)
    aggregate_b = aggregate.astype(jnp.bfloat16)
    node_pre = jnp.dot(node_latent, w_node, preferred_element_type=jnp.float32) + jnp.dot(aggregate_b, w_agg, preferred_element_type=jnp.float32) + node_bias
    node_hidden = jax.nn.silu(node_pre).astype(jnp.bfloat16)
    node_message = jnp.dot(node_hidden, node_out, preferred_element_type=jnp.float32) + node_out_bias
    new_node = (node_latent.astype(jnp.float32) + layer_norm(node_message, node_gain, node_offset)).astype(jnp.bfloat16)
    return (new_edge, new_node)
```

```python
import functools

import jax
import jax.numpy as jnp
from jax import lax
from jax.experimental import pallas as pl
from jax.experimental.pallas import tpu as pltpu
from jax.sharding import PartitionSpec as P

MESH = pl.DeviceIdType.MESH
LANES = 128
F32 = jnp.float32
BF16 = jnp.bfloat16
EPS = 1e-05


def round_up(count, unit):
    return (count + unit - 1) // unit * unit


def dot(left, right):
    return jnp.dot(left, right, preferred_element_type=F32)


def silu(values):
    half = 0.5 * values
    return half + half * jnp.tanh(half)


def layer_norm(values, gain, offset):
    scale = 1.0 / values.shape[-1]
    mean = jnp.sum(values, axis=-1, keepdims=True) * scale
    centered = values - mean
    spread = jnp.sum(centered * centered, axis=-1, keepdims=True) * scale
    return centered * lax.rsqrt(spread + EPS) * gain + offset


def onehot_rows(row, width):
    blocks = []
    for start in range(0, row.shape[1], LANES):
        piece = row[:, start : start + LANES]
        column = jnp.transpose(jnp.broadcast_to(piece, (LANES, LANES)))
        lane = lax.broadcasted_iota(jnp.int32, (LANES, LANES), 1)
        parts = [
            jnp.where(column == lane + first, 1.0, 0.0).astype(BF16)
            for first in range(0, width, LANES)
        ]
        blocks.append(jnp.concatenate(parts, axis=1))
    return jnp.concatenate(blocks, axis=0)


def kernel(
    patches,
    tile,
    early,
    count_ref,
    send_rows_ref,
    sender_ref,
    receiver_ref,
    edge_bias_ref,
    edge_out_bias_ref,
    edge_gain_ref,
    edge_offset_ref,
    node_bias_ref,
    node_out_bias_ref,
    node_gain_ref,
    node_offset_ref,
    node_hbm,
    edge_hbm,
    w_edge_hbm,
    w_send_hbm,
    w_recv_hbm,
    edge_out_hbm,
    w_node_hbm,
    w_agg_hbm,
    node_out_hbm,
    new_edge_hbm,
    new_node_ref,
    node,
    edges,
    first_table,
    w_send,
    w_recv,
    edge_out,
    w_node,
    w_agg,
    node_out,
    outgoing,
    arrived,
    send_table,
    part,
    send_hot,
    recv_hot,
    updated,
    aggregate,
    agg_mine,
    agg_other,
    node_part,
    load_sem,
    edge_sem,
    store_sem,
    send_sem,
    recv_sem,
    pass_sem,
    passed_sem,
    agg_sem,
):
    me = lax.axis_index("patch")
    core = lax.axis_index("pair")
    other = 1 - core
    nodes, width = node_hbm.shape
    padded = node.shape[0]
    edge_rows = edge_hbm.shape[0]
    tiles = edge_rows // tile
    slots, half = outgoing.shape[1:]
    barrier = pltpu.get_barrier_semaphore()

    def greet(step, carry):
        pl.semaphore_signal(
            barrier, inc=1, device_id=(lax.rem(me + step, patches), core), device_id_type=MESH
        )
        return carry

    lax.fori_loop(1, patches, greet, 0)
    pl.semaphore_signal(barrier, inc=1, device_id=(me, other), device_id_type=MESH)

    loads = [
        pltpu.make_async_copy(source, target, load_sem.at[number])
        for number, (source, target) in enumerate(
            (
                (node_hbm, node.at[pl.ds(0, nodes)]),
                (w_recv_hbm, w_recv),
                (w_edge_hbm, first_table.at[pl.ds(0, width)]),
                (w_node_hbm, w_node),
                (w_send_hbm, w_send),
                (edge_out_hbm, edge_out),
                (w_agg_hbm, w_agg),
                (node_out_hbm, node_out),
            )
        )
    ]

    def edge_load(index):
        rows = pl.ds(index * tile, tile)
        return pltpu.make_async_copy(edge_hbm.at[rows], edges.at[rows], edge_sem.at[index])

    for load in loads[:3]:
        load.start()
    for index in range(tiles):
        edge_load(index).start()
    for load in loads[3:]:
        load.start()

    if padded > nodes:
        node[pl.ds(nodes, padded - nodes), :] = jnp.zeros((padded - nodes, width), BF16)
    loads[0].wait()
    columns = pl.ds(pl.multiple_of(core * half, LANES), half)
    block = max(1, LANES // slots)
    for first in range(0, patches, block):
        hot = onehot_rows(send_rows_ref[:, first * slots : (first + block) * slots], padded)
        picked = dot(hot, node[:, columns]).astype(BF16)
        outgoing[first : first + block] = picked.reshape(block, slots, half)

    loads[1].wait()
    first_table[pl.ds(width, padded), :] = dot(node[...], w_recv[...]).astype(BF16)
    loads[2].wait()

    def first_layer(index, carry):
        rows = pl.ds(pl.multiple_of(index * tile, tile), tile)
        edge_load(index).wait()
        receiver = receiver_ref[:, rows]
        hot = onehot_rows(receiver, padded)
        left = jnp.concatenate([edges[rows, :], hot], axis=1)
        part[rows, :] = dot(left, first_table[...]) + edge_bias_ref[...]
        send_hot[rows, :] = onehot_rows(sender_ref[:, rows], send_hot.shape[1])
        ids = lax.broadcasted_iota(jnp.int32, (nodes, tile), 0)
        recv_hot[:, rows] = jnp.where(ids == receiver, 1.0, 0.0).astype(BF16)
        return carry

    lax.fori_loop(0, early, first_layer, 0)

    pl.semaphore_wait(barrier, patches)

    def to_patch(step):
        target = lax.rem(me + step, patches)
        return pltpu.make_async_remote_copy(
            src_ref=outgoing.at[target],
            dst_ref=arrived.at[core, me],
            send_sem=send_sem.at[target],
            recv_sem=recv_sem.at[me],
            device_id=(target, core),
            device_id_type=MESH,
        )

    def from_patch(source):
        return pltpu.make_async_remote_copy(
            src_ref=outgoing.at[source],
            dst_ref=arrived.at[core, source],
            send_sem=send_sem.at[source],
            recv_sem=recv_sem.at[source],
            device_id=(source, core),
            device_id_type=MESH,
        )

    def to_core(source, source_ref):
        return pltpu.make_async_remote_copy(
            src_ref=source_ref,
            dst_ref=arrived.at[core, source],
            send_sem=pass_sem.at[source],
            recv_sem=passed_sem.at[source],
            device_id=(me, other),
            device_id_type=MESH,
        )

    def from_core(source):
        return pltpu.make_async_remote_copy(
            src_ref=arrived.at[core, source],
            dst_ref=arrived.at[other, source],
            send_sem=pass_sem.at[source],
            recv_sem=passed_sem.at[source],
            device_id=(me, other),
            device_id_type=MESH,
        )

    def send_step(step, carry):
        to_patch(step).start()
        return carry

    lax.fori_loop(1, patches, send_step, 0)
    to_core(me, outgoing.at[me]).start()
    arrived[core, me] = outgoing[me]

    lax.fori_loop(early, tiles, first_layer, 0)

    for load in loads[3:]:
        load.wait()
    node_part[...] = dot(node[pl.ds(0, nodes), :], w_node[...]) + node_bias_ref[...]
    aggregate[...] = jnp.zeros_like(aggregate)

    def pass_step(step, carry):
        source = lax.rem(me + patches - step, patches)
        from_patch(source).wait_recv()
        to_core(source, arrived.at[core, source]).start()
        return carry

    lax.fori_loop(1, patches, pass_step, 0)

    def passed_step(step, carry):
        from_core(lax.rem(me + patches - step, patches)).wait_recv()
        return carry

    lax.fori_loop(0, patches, passed_step, 0)
    for first in range(0, patches, block):
        rows = jnp.concatenate(
            [arrived[side, first : first + block].reshape(block * slots, half) for side in range(2)],
            axis=1,
        )
        send_table[first * slots : (first + block) * slots, :] = dot(rows, w_send[...]).astype(BF16)

    count = count_ref[0]

    def store(index):
        rows = pl.ds(pl.multiple_of(index * tile, tile), tile)
        return pltpu.make_async_copy(updated.at[rows], new_edge_hbm.at[rows], store_sem.at[index])

    def second_layer(index, carry):
        rows = pl.ds(pl.multiple_of(index * tile, tile), tile)
        pre = part[rows, :] + dot(send_hot[rows, :], send_table[...])
        hidden = silu(pre).astype(BF16)
        message = dot(hidden, edge_out[...]) + edge_out_bias_ref[...]
        delta = layer_norm(message, edge_gain_ref[...], edge_offset_ref[...])
        ids = lax.broadcasted_iota(jnp.int32, (tile, width), 0) + index * tile
        delta = jnp.where(ids < count, delta, 0.0).astype(BF16)
        updated[rows, :] = (edges[rows, :].astype(F32) + delta.astype(F32)).astype(BF16)
        store(index).start()
        aggregate[...] += dot(recv_hot[:, rows], delta)
        return carry

    lax.fori_loop(0, tiles, second_layer, 0)

    agg_mine[...] = aggregate[...].astype(BF16)
    exchange = pltpu.make_async_remote_copy(
        src_ref=agg_mine,
        dst_ref=agg_other,
        send_sem=agg_sem.at[0],
        recv_sem=agg_sem.at[1],
        device_id=(me, other),
        device_id_type=MESH,
    )
    exchange.start()

    def sent_step(step, carry):
        to_patch(step).wait_send()
        source = lax.rem(me + step, patches)
        to_core(source, arrived.at[core, source]).wait_send()
        return carry

    lax.fori_loop(1, patches, sent_step, 0)
    to_core(me, outgoing.at[me]).wait_send()
    exchange.wait()

    summed = (agg_mine[...].astype(F32) + agg_other[...].astype(F32)).astype(BF16)
    hidden = silu(node_part[...] + dot(summed, w_agg[...])).astype(BF16)
    message = dot(hidden, node_out[...]) + node_out_bias_ref[...]
    normed = layer_norm(message, node_gain_ref[...], node_offset_ref[...])
    new_node_ref[...] = (node[pl.ds(0, nodes), :].astype(F32) + normed).astype(BF16)

    def stored_step(index, carry):
        store(index).wait()
        return carry

    lax.fori_loop(0, tiles, stored_step, 0)


def on_device(
    patches,
    node_latent,
    edge_latent,
    edge_sender,
    edge_receiver,
    edge_count,
    send_rows,
    w_edge,
    w_send,
    w_recv,
    edge_bias,
    edge_out,
    edge_out_bias,
    edge_gain,
    edge_offset,
    w_node,
    w_agg,
    node_bias,
    node_out,
    node_out_bias,
    node_gain,
    node_offset,
):
    nodes, width = node_latent.shape
    edge_rows = edge_latent.shape[0]
    slots = send_rows.shape[2]
    senders = patches * slots
    padded = round_up(nodes, LANES)
    half = width // 2
    tile = 256
    early = 2
    tiles = edge_rows // tile
    vmem = pl.BlockSpec(memory_space=pltpu.VMEM)
    smem = pl.BlockSpec(memory_space=pltpu.SMEM)
    hbm = pl.BlockSpec(memory_space=pl.ANY)
    weight = pltpu.VMEM((width, width), BF16)
    return pl.pallas_call(
        functools.partial(kernel, patches, tile, early),
        out_shape=(
            jax.ShapeDtypeStruct(edge_latent.shape, BF16),
            jax.ShapeDtypeStruct(node_latent.shape, BF16),
        ),
        in_specs=[smem] + [vmem] * 11 + [hbm] * 9,
        out_specs=(hbm, vmem),
        scratch_shapes=[
            pltpu.VMEM((padded, width), BF16),
            pltpu.VMEM((edge_rows, width), BF16),
            pltpu.VMEM((width + padded, width), BF16),
            weight,
            weight,
            weight,
            weight,
            weight,
            weight,
            pltpu.VMEM((patches, slots, half), BF16),
            pltpu.VMEM((2, patches, slots, half), BF16),
            pltpu.VMEM((senders, width), BF16),
            pltpu.VMEM((edge_rows, width), F32),
            pltpu.VMEM((edge_rows, senders), BF16),
            pltpu.VMEM((nodes, edge_rows), BF16),
            pltpu.VMEM((edge_rows, width), BF16),
            pltpu.VMEM((nodes, width), F32),
            pltpu.VMEM((nodes, width), BF16),
            pltpu.VMEM((nodes, width), BF16),
            pltpu.VMEM((nodes, width), F32),
            pltpu.SemaphoreType.DMA((8,)),
            pltpu.SemaphoreType.DMA((tiles,)),
            pltpu.SemaphoreType.DMA((tiles,)),
            pltpu.SemaphoreType.DMA((patches,)),
            pltpu.SemaphoreType.DMA((patches,)),
            pltpu.SemaphoreType.DMA((patches,)),
            pltpu.SemaphoreType.DMA((patches,)),
            pltpu.SemaphoreType.DMA((2,)),
        ],
        compiler_params=pltpu.CompilerParams(
            collective_id=0, has_side_effects=True, vmem_limit_bytes=60 * 1024 * 1024
        ),
    )(
        edge_count,
        send_rows.reshape(1, senders),
        edge_sender.reshape(1, edge_rows),
        edge_receiver.reshape(1, edge_rows),
        edge_bias.reshape(1, width),
        edge_out_bias.reshape(1, width),
        edge_gain.reshape(1, width),
        edge_offset.reshape(1, width),
        node_bias.reshape(1, width),
        node_out_bias.reshape(1, width),
        node_gain.reshape(1, width),
        node_offset.reshape(1, width),
        node_latent,
        edge_latent,
        w_edge,
        w_send,
        w_recv,
        edge_out,
        w_node,
        w_agg,
        node_out,
    )


def solution(mesh):
    placed = (
        P("patch", None),
        P(("patch", "pair"), None),
        P(("patch", "pair")),
        P(("patch", "pair")),
        P(("patch", "pair")),
        P("patch", None, None),
    ) + (P(),) * 15
    return jax.shard_map(
        functools.partial(on_device, mesh.shape["patch"]),
        mesh=mesh,
        in_specs=placed,
        out_specs=(P(("patch", "pair"), None), P("patch", None)),
        check_vma=False,
    )
```

```python
import functools

import jax
import jax.numpy as jnp
from jax import lax
from jax.experimental import pallas as pl
from jax.experimental.pallas import tpu as pltpu
from jax.sharding import PartitionSpec as P

MESH = pl.DeviceIdType.MESH
LANES = 128
F32 = jnp.float32
BF16 = jnp.bfloat16
EPS = 1e-05


def round_up(count, unit):
    return (count + unit - 1) // unit * unit


def dot(left, right):
    return jnp.dot(left, right, preferred_element_type=F32)


def silu(values):
    half = 0.5 * values
    return half + half * jnp.tanh(half)


def layer_norm(values, gain, offset):
    scale = 1.0 / values.shape[-1]
    mean = jnp.sum(values, axis=-1, keepdims=True) * scale
    centered = values - mean
    spread = jnp.sum(centered * centered, axis=-1, keepdims=True) * scale
    return centered * lax.rsqrt(spread + EPS) * gain + offset


def onehot_rows(row, width):
    blocks = []
    for start in range(0, row.shape[1], LANES):
        piece = row[:, start : start + LANES]
        column = jnp.transpose(jnp.broadcast_to(piece, (LANES, LANES)))
        lane = lax.broadcasted_iota(jnp.int32, (LANES, LANES), 1)
        parts = [
            jnp.where(column == lane + first, 1.0, 0.0).astype(BF16)
            for first in range(0, width, LANES)
        ]
        blocks.append(jnp.concatenate(parts, axis=1))
    return jnp.concatenate(blocks, axis=0)


def onehot_slots(rows, width):
    count, slots = rows.shape
    eye = lax.broadcasted_iota(jnp.int32, (slots, slots), 0) == lax.broadcasted_iota(
        jnp.int32, (slots, slots), 1
    )
    picked = [
        jnp.where(eye, jnp.broadcast_to(rows[at : at + 1], (slots, slots)), 0)
        for at in range(count)
    ]
    column = jnp.sum(jnp.concatenate(picked, axis=0).astype(F32), axis=1, keepdims=True)
    lane = lax.broadcasted_iota(jnp.int32, (count * slots, LANES), 1).astype(F32)
    return jnp.concatenate(
        [jnp.where(column == lane + first, 1.0, 0.0).astype(BF16) for first in range(0, width, LANES)],
        axis=1,
    )


def edge_kernel(
    patches,
    tile,
    early,
    chunk,
    pieces,
    count_ref,
    send_rows_hbm,
    sender_hbm,
    receiver_hbm,
    edge_bias_hbm,
    edge_out_bias_hbm,
    edge_gain_hbm,
    edge_offset_hbm,
    node_hbm,
    edge_hbm,
    w_edge_hbm,
    w_send_hbm,
    w_recv_hbm,
    edge_out_hbm,
    new_edge_hbm,
    summed_ref,
    send_rows_ref,
    sender_ref,
    receiver_ref,
    edge_bias_ref,
    edge_out_bias_ref,
    edge_gain_ref,
    edge_offset_ref,
    node,
    edges,
    first_table,
    w_send,
    w_recv,
    edge_out,
    outgoing,
    arrived,
    send_table,
    part,
    send_hot,
    recv_hot,
    updated,
    aggregate,
    agg_mine,
    agg_other,
    load_sem,
    edge_sem,
    store_sem,
    send_sem,
    recv_sem,
    pass_sem,
    passed_sem,
    agg_sem,
):
    me = lax.axis_index("patch")
    core = lax.axis_index("pair")
    other = 1 - core
    nodes, width = node_hbm.shape
    padded = node.shape[0]
    edge_rows = edge_hbm.shape[0]
    tiles = edge_rows // tile
    slots, half = outgoing.shape[1:]
    barrier = pltpu.get_barrier_semaphore()

    loads = [
        pltpu.make_async_copy(source, target, load_sem.at[number])
        for number, (source, target) in enumerate(
            (
                (node_hbm, node.at[pl.ds(0, nodes)]),
                (send_rows_hbm, send_rows_ref),
                (w_recv_hbm, w_recv),
                (w_edge_hbm, first_table.at[pl.ds(0, width)]),
                (sender_hbm, sender_ref),
                (receiver_hbm, receiver_ref),
                (edge_bias_hbm, edge_bias_ref),
                (w_send_hbm, w_send),
                (edge_out_hbm, edge_out),
                (edge_out_bias_hbm, edge_out_bias_ref),
                (edge_gain_hbm, edge_gain_ref),
                (edge_offset_hbm, edge_offset_ref),
            )
        )
    ]
    for load in loads[:2]:
        load.start()

    def far_first(at, ends):
        low, high = ends
        take_low = me - low > high - me
        target = jnp.where(take_low, low, high)
        return target, (jnp.where(take_low, low + 1, low), jnp.where(take_low, high, high - 1))

    def greet(at, ends):
        target, ends = far_first(at, ends)
        pl.semaphore_signal(barrier, inc=1, device_id=(target, core), device_id_type=MESH)
        return ends

    ends = (jnp.int32(0), jnp.int32(patches - 1))
    lax.fori_loop(1, patches, greet, ends)
    pl.semaphore_signal(barrier, inc=1, device_id=(me, other), device_id_type=MESH)

    def edge_load(index):
        rows = pl.ds(index * tile, tile)
        return pltpu.make_async_copy(edge_hbm.at[rows], edges.at[rows], edge_sem.at[index])

    for load in loads[2:7]:
        load.start()
    for index in range(tiles):
        edge_load(index).start()
    for load in loads[7:]:
        load.start()

    if padded > nodes:
        node[pl.ds(nodes, padded - nodes), :] = jnp.zeros((padded - nodes, width), BF16)
    loads[0].wait()
    loads[1].wait()
    columns = pl.ds(pl.multiple_of(core * half, LANES), half)
    block = max(1, LANES // slots)
    for first in range(0, patches, block):
        hot = onehot_slots(send_rows_ref[first : first + block, :], padded)
        picked = dot(hot, node[:, columns]).astype(BF16)
        outgoing[first : first + block] = picked.reshape(block, slots, half)

    loads[2].wait()
    first_table[pl.ds(width, padded), :] = dot(node[...], w_recv[...]).astype(BF16)
    for load in loads[3:7]:
        load.wait()

    def first_layer(index, carry):
        rows = pl.ds(pl.multiple_of(index * tile, tile), tile)
        edge_load(index).wait()
        receiver = receiver_ref[:, rows]
        hot = onehot_rows(receiver, padded)
        left = jnp.concatenate([edges[rows, :], hot], axis=1)
        part[rows, :] = dot(left, first_table[...]) + edge_bias_ref[...]
        send_hot[rows, :] = onehot_rows(sender_ref[:, rows], send_hot.shape[1])
        ids = lax.broadcasted_iota(jnp.int32, (nodes, tile), 0)
        recv_hot[:, rows] = jnp.where(ids == receiver, 1.0, 0.0).astype(BF16)
        return carry

    lax.fori_loop(0, early, first_layer, 0)

    pl.semaphore_wait(barrier, patches)

    def to_patch(target):
        return pltpu.make_async_remote_copy(
            src_ref=outgoing.at[target],
            dst_ref=arrived.at[core, me],
            send_sem=send_sem.at[target],
            recv_sem=recv_sem.at[me],
            device_id=(target, core),
            device_id_type=MESH,
        )

    def from_patch(source):
        return pltpu.make_async_remote_copy(
            src_ref=outgoing.at[source],
            dst_ref=arrived.at[core, source],
            send_sem=send_sem.at[source],
            recv_sem=recv_sem.at[source],
            device_id=(source, core),
            device_id_type=MESH,
        )

    def to_core(source, source_ref):
        return pltpu.make_async_remote_copy(
            src_ref=source_ref,
            dst_ref=arrived.at[core, source],
            send_sem=pass_sem.at[source],
            recv_sem=passed_sem.at[source],
            device_id=(me, other),
            device_id_type=MESH,
        )

    def from_core(source):
        return pltpu.make_async_remote_copy(
            src_ref=arrived.at[core, source],
            dst_ref=arrived.at[other, source],
            send_sem=pass_sem.at[source],
            recv_sem=passed_sem.at[source],
            device_id=(me, other),
            device_id_type=MESH,
        )

    def send_step(at, ends):
        target, ends = far_first(at, ends)
        to_patch(target).start()
        return ends

    lax.fori_loop(1, patches, send_step, ends)
    to_core(me, outgoing.at[me]).start()
    arrived[core, me] = outgoing[me]

    lax.fori_loop(early, tiles, first_layer, 0)

    for load in loads[7:]:
        load.wait()
    aggregate[...] = jnp.zeros_like(aggregate)

    def pass_step(step, carry):
        source = lax.rem(me + patches - step, patches)
        from_patch(source).wait_recv()
        to_core(source, arrived.at[core, source]).start()
        return carry

    lax.fori_loop(1, patches, pass_step, 0)

    def passed_step(step, carry):
        from_core(lax.rem(me + patches - step, patches)).wait_recv()
        return carry

    lax.fori_loop(0, patches, passed_step, 0)
    for first in range(0, patches, block):
        rows = jnp.concatenate(
            [arrived[side, first : first + block].reshape(block * slots, half) for side in range(2)],
            axis=1,
        )
        send_table[first * slots : (first + block) * slots, :] = dot(rows, w_send[...]).astype(BF16)

    count = count_ref[0]

    def store(index):
        rows = pl.ds(pl.multiple_of(index * chunk, chunk), chunk)
        return pltpu.make_async_copy(updated.at[rows], new_edge_hbm.at[rows], store_sem.at[index])

    def second_layer(index, carry):
        span = chunk // pieces
        deltas = []
        for piece in range(pieces):
            first = pl.multiple_of(index * chunk, chunk) + piece * span
            rows = pl.ds(first, span)
            pre = part[rows, :] + dot(send_hot[rows, :], send_table[...])
            hidden = silu(pre).astype(BF16)
            message = dot(hidden, edge_out[...]) + edge_out_bias_ref[...]
            delta = layer_norm(message, edge_gain_ref[...], edge_offset_ref[...])
            ids = lax.broadcasted_iota(jnp.int32, (span, width), 0) + first
            delta = jnp.where(ids < count, delta, 0.0).astype(BF16)
            updated[rows, :] = (edges[rows, :].astype(F32) + delta.astype(F32)).astype(BF16)
            deltas.append(delta)
        store(index).start()
        rows = pl.ds(pl.multiple_of(index * chunk, chunk), chunk)
        aggregate[...] += dot(recv_hot[:, rows], jnp.concatenate(deltas, axis=0))
        return carry

    chunks = edge_rows // chunk
    lax.fori_loop(0, chunks, second_layer, 0)

    agg_mine[...] = aggregate[...].astype(BF16)
    exchange = pltpu.make_async_remote_copy(
        src_ref=agg_mine,
        dst_ref=agg_other,
        send_sem=agg_sem.at[0],
        recv_sem=agg_sem.at[1],
        device_id=(me, other),
        device_id_type=MESH,
    )
    exchange.start()

    def sent_step(step, carry):
        source = lax.rem(me + step, patches)
        to_patch(source).wait_send()
        to_core(source, arrived.at[core, source]).wait_send()
        return carry

    lax.fori_loop(1, patches, sent_step, 0)
    to_core(me, outgoing.at[me]).wait_send()

    def stored_step(index, carry):
        store(index).wait()
        return carry

    lax.fori_loop(0, chunks, stored_step, 0)
    exchange.wait()
    summed_ref[...] = (agg_mine[...].astype(F32) + agg_other[...].astype(F32)).astype(BF16)


def node_kernel(
    pieces,
    node_bias_ref,
    node_out_bias_ref,
    node_gain_ref,
    node_offset_ref,
    summed_hbm,
    node_hbm,
    w_node_hbm,
    w_agg_hbm,
    node_out_hbm,
    edge_hbm,
    new_edge_hbm,
    new_node_ref,
    summed,
    node,
    w_node,
    w_agg,
    node_out,
    edges,
    load_sem,
    in_sem,
    out_sem,
):
    rows = edge_hbm.shape[0] // pieces
    loads = [
        pltpu.make_async_copy(source, target, load_sem.at[number])
        for number, (source, target) in enumerate(
            (
                (node_hbm, node),
                (w_node_hbm, w_node),
                (summed_hbm, summed),
                (w_agg_hbm, w_agg),
                (node_out_hbm, node_out),
            )
        )
    ]
    takes = [
        pltpu.make_async_copy(
            edge_hbm.at[pl.ds(at * rows, rows)], edges.at[pl.ds(at * rows, rows)], in_sem.at[at]
        )
        for at in range(pieces)
    ]
    puts = [
        pltpu.make_async_copy(
            edges.at[pl.ds(at * rows, rows)], new_edge_hbm.at[pl.ds(at * rows, rows)], out_sem.at[at]
        )
        for at in range(pieces)
    ]
    for copy in takes + loads:
        copy.start()
    for take, put in zip(takes, puts):
        take.wait()
        put.start()
    for load in loads:
        load.wait()
    node_pre = dot(node[...], w_node[...]) + dot(summed[...], w_agg[...]) + node_bias_ref[...]
    hidden = silu(node_pre).astype(BF16)
    message = dot(hidden, node_out[...]) + node_out_bias_ref[...]
    normed = layer_norm(message, node_gain_ref[...], node_offset_ref[...])
    new_node_ref[...] = (node[...].astype(F32) + normed).astype(BF16)
    for put in puts:
        put.wait()


def on_device(
    patches,
    node_latent,
    edge_latent,
    edge_sender,
    edge_receiver,
    edge_count,
    send_rows,
    w_edge,
    w_send,
    w_recv,
    edge_bias,
    edge_out,
    edge_out_bias,
    edge_gain,
    edge_offset,
    w_node,
    w_agg,
    node_bias,
    node_out,
    node_out_bias,
    node_gain,
    node_offset,
):
    nodes, width = node_latent.shape
    edge_rows = edge_latent.shape[0]
    slots = send_rows.shape[2]
    senders = patches * slots
    padded = round_up(nodes, LANES)
    half = width // 2
    tile = 256
    early = 2
    chunk = 512
    pieces = 1
    tiles = edge_rows // tile
    vmem = pl.BlockSpec(memory_space=pltpu.VMEM)
    smem = pl.BlockSpec(memory_space=pltpu.SMEM)
    hbm = pl.BlockSpec(memory_space=pl.ANY)
    weight = pltpu.VMEM((width, width), BF16)
    vector = pltpu.VMEM((1, width), F32)
    scratch = [
        pltpu.VMEM((patches, slots), jnp.int32),
        pltpu.VMEM((1, edge_rows), jnp.int32),
        pltpu.VMEM((1, edge_rows), jnp.int32),
        vector,
        vector,
        vector,
        vector,
        pltpu.VMEM((padded, width), BF16),
        pltpu.VMEM((edge_rows, width), BF16),
        pltpu.VMEM((width + padded, width), BF16),
        weight,
        weight,
        weight,
        pltpu.VMEM((patches, slots, half), BF16),
        pltpu.VMEM((2, patches, slots, half), BF16),
        pltpu.VMEM((senders, width), BF16),
        pltpu.VMEM((edge_rows, width), F32),
        pltpu.VMEM((edge_rows, senders), BF16),
        pltpu.VMEM((nodes, edge_rows), BF16),
        pltpu.VMEM((edge_rows, width), BF16),
        pltpu.VMEM((nodes, width), F32),
        pltpu.VMEM((nodes, width), BF16),
        pltpu.VMEM((nodes, width), BF16),
    ]
    edge_flops = 2 * edge_rows * width * (2 * width + senders + padded + nodes)
    edge_new, summed = pl.pallas_call(
        functools.partial(edge_kernel, patches, tile, early, chunk, pieces),
        out_shape=(
            jax.ShapeDtypeStruct(edge_latent.shape, BF16),
            jax.ShapeDtypeStruct(node_latent.shape, BF16),
        ),
        in_specs=[smem] + [hbm] * 13,
        out_specs=(hbm, vmem),
        scratch_shapes=scratch
        + [
            pltpu.SemaphoreType.DMA((12,)),
            pltpu.SemaphoreType.DMA((tiles,)),
            pltpu.SemaphoreType.DMA((edge_rows // chunk,)),
            pltpu.SemaphoreType.DMA((patches,)),
            pltpu.SemaphoreType.DMA((patches,)),
            pltpu.SemaphoreType.DMA((patches,)),
            pltpu.SemaphoreType.DMA((patches,)),
            pltpu.SemaphoreType.DMA((2,)),
        ],
        cost_estimate=pl.CostEstimate(
            flops=edge_flops, bytes_accessed=4 * edge_rows * width, transcendentals=0
        ),
        compiler_params=pltpu.CompilerParams(
            collective_id=0, has_side_effects=True, vmem_limit_bytes=62 * 1024 * 1024
        ),
    )(
        edge_count,
        send_rows.reshape(patches, slots),
        edge_sender.reshape(1, edge_rows),
        edge_receiver.reshape(1, edge_rows),
        edge_bias.reshape(1, width),
        edge_out_bias.reshape(1, width),
        edge_gain.reshape(1, width),
        edge_offset.reshape(1, width),
        node_latent,
        edge_latent,
        w_edge,
        w_send,
        w_recv,
        edge_out,
    )
    node_pieces = 4
    rows = pltpu.VMEM((nodes, width), BF16)
    return pl.pallas_call(
        functools.partial(node_kernel, node_pieces),
        out_shape=(
            jax.ShapeDtypeStruct(edge_latent.shape, BF16),
            jax.ShapeDtypeStruct(node_latent.shape, BF16),
        ),
        in_specs=[vmem] * 4 + [hbm] * 6,
        out_specs=(hbm, vmem),
        scratch_shapes=[
            rows,
            rows,
            weight,
            weight,
            weight,
            pltpu.VMEM((edge_rows, width), BF16),
            pltpu.SemaphoreType.DMA((5,)),
            pltpu.SemaphoreType.DMA((node_pieces,)),
            pltpu.SemaphoreType.DMA((node_pieces,)),
        ],
        compiler_params=pltpu.CompilerParams(vmem_limit_bytes=60 * 1024 * 1024),
    )(
        node_bias.reshape(1, width),
        node_out_bias.reshape(1, width),
        node_gain.reshape(1, width),
        node_offset.reshape(1, width),
        summed,
        node_latent,
        w_node,
        w_agg,
        node_out,
        edge_new,
    )


def solution(mesh):
    placed = (
        P("patch", None),
        P(("patch", "pair"), None),
        P(("patch", "pair")),
        P(("patch", "pair")),
        P(("patch", "pair")),
        P("patch", None, None),
    ) + (P(),) * 15
    return jax.shard_map(
        functools.partial(on_device, mesh.shape["patch"]),
        mesh=mesh,
        in_specs=placed,
        out_specs=(P(("patch", "pair"), None), P("patch", None)),
        check_vma=False,
    )
```

```python
import functools

import jax
import jax.numpy as jnp
from jax import lax
from jax.experimental import pallas as pl
from jax.experimental.pallas import tpu as pltpu
from jax.sharding import PartitionSpec as P

MESH = pl.DeviceIdType.MESH
LANES = 128
F32 = jnp.float32
BF16 = jnp.bfloat16
EPS = 1e-05


def round_up(count, unit):
    return (count + unit - 1) // unit * unit


def dot(left, right):
    return jnp.dot(left, right, preferred_element_type=F32)


def silu(values):
    half = 0.5 * values
    return half + half * jnp.tanh(half)


def layer_norm(values, gain, offset):
    scale = 1.0 / values.shape[-1]
    mean = jnp.sum(values, axis=-1, keepdims=True) * scale
    centered = values - mean
    spread = jnp.sum(centered * centered, axis=-1, keepdims=True) * scale
    return centered * lax.rsqrt(spread + EPS) * gain + offset


def onehot_rows(row, width):
    blocks = []
    for start in range(0, row.shape[1], LANES):
        piece = row[:, start : start + LANES]
        column = jnp.transpose(jnp.broadcast_to(piece, (LANES, LANES)))
        lane = lax.broadcasted_iota(jnp.int32, (LANES, LANES), 1)
        parts = [
            jnp.where(column == lane + first, 1.0, 0.0).astype(BF16)
            for first in range(0, width, LANES)
        ]
        blocks.append(jnp.concatenate(parts, axis=1))
    return jnp.concatenate(blocks, axis=0)


def onehot_slots(rows, width):
    count, slots = rows.shape
    eye = lax.broadcasted_iota(jnp.int32, (slots, slots), 0) == lax.broadcasted_iota(
        jnp.int32, (slots, slots), 1
    )
    picked = [
        jnp.where(eye, jnp.broadcast_to(rows[at : at + 1], (slots, slots)), 0)
        for at in range(count)
    ]
    column = jnp.sum(jnp.concatenate(picked, axis=0).astype(F32), axis=1, keepdims=True)
    lane = lax.broadcasted_iota(jnp.int32, (count * slots, LANES), 1).astype(F32)
    return jnp.concatenate(
        [jnp.where(column == lane + first, 1.0, 0.0).astype(BF16) for first in range(0, width, LANES)],
        axis=1,
    )


def edge_kernel(
    patches,
    tile,
    chunk,
    pieces,
    count_ref,
    send_rows_hbm,
    sender_hbm,
    receiver_hbm,
    edge_bias_hbm,
    edge_out_bias_hbm,
    edge_gain_hbm,
    edge_offset_hbm,
    node_hbm,
    edge_hbm,
    w_edge_hbm,
    w_send_hbm,
    w_recv_hbm,
    edge_out_hbm,
    new_edge_hbm,
    summed_ref,
    send_rows_ref,
    sender_ref,
    receiver_ref,
    edge_bias_ref,
    edge_out_bias_ref,
    edge_gain_ref,
    edge_offset_ref,
    node,
    edges,
    first_table,
    w_send,
    w_recv,
    edge_out,
    outgoing,
    arrived,
    send_table,
    part,
    send_hot,
    recv_hot,
    updated,
    aggregate,
    agg_mine,
    agg_other,
    load_sem,
    edge_sem,
    store_sem,
    send_sem,
    recv_sem,
    pass_sem,
    passed_sem,
    agg_sem,
):
    me = lax.axis_index("patch")
    core = lax.axis_index("pair")
    other = 1 - core
    nodes, width = node_hbm.shape
    padded = node.shape[0]
    edge_rows = edge_hbm.shape[0]
    tiles = edge_rows // tile
    slots, half = outgoing.shape[1:]
    barrier = pltpu.get_barrier_semaphore()

    loads = [
        pltpu.make_async_copy(source, target, load_sem.at[number])
        for number, (source, target) in enumerate(
            (
                (node_hbm, node.at[pl.ds(0, nodes)]),
                (send_rows_hbm, send_rows_ref),
                (w_recv_hbm, w_recv),
                (w_edge_hbm, first_table.at[pl.ds(0, width)]),
                (sender_hbm, sender_ref),
                (receiver_hbm, receiver_ref),
                (edge_bias_hbm, edge_bias_ref),
                (w_send_hbm, w_send),
                (edge_out_hbm, edge_out),
                (edge_out_bias_hbm, edge_out_bias_ref),
                (edge_gain_hbm, edge_gain_ref),
                (edge_offset_hbm, edge_offset_ref),
            )
        )
    ]
    for load in loads[:2]:
        load.start()

    def far_first(at, ends):
        low, high = ends
        take_low = me - low > high - me
        target = jnp.where(take_low, low, high)
        return target, (jnp.where(take_low, low + 1, low), jnp.where(take_low, high, high - 1))

    def greet(at, ends):
        target, ends = far_first(at, ends)
        pl.semaphore_signal(barrier, inc=1, device_id=(target, core), device_id_type=MESH)
        return ends

    ends = (jnp.int32(0), jnp.int32(patches - 1))
    lax.fori_loop(1, patches, greet, ends)
    pl.semaphore_signal(barrier, inc=1, device_id=(me, other), device_id_type=MESH)

    def edge_load(index):
        rows = pl.ds(index * tile, tile)
        return pltpu.make_async_copy(edge_hbm.at[rows], edges.at[rows], edge_sem.at[index])

    for load in loads[2:7]:
        load.start()
    for index in range(tiles):
        edge_load(index).start()
    for load in loads[7:]:
        load.start()

    if padded > nodes:
        node[pl.ds(nodes, padded - nodes), :] = jnp.zeros((padded - nodes, width), BF16)
    loads[0].wait()
    loads[1].wait()
    columns = pl.ds(pl.multiple_of(core * half, LANES), half)
    block = max(1, LANES // slots)
    for first in range(0, patches, block):
        hot = onehot_slots(send_rows_ref[first : first + block, :], padded)
        picked = dot(hot, node[:, columns]).astype(BF16)
        outgoing[first : first + block] = picked.reshape(block, slots, half)


    def first_layer(index, carry):
        rows = pl.ds(pl.multiple_of(index * tile, tile), tile)
        edge_load(index).wait()
        receiver = receiver_ref[:, rows]
        hot = onehot_rows(receiver, padded)
        left = jnp.concatenate([edges[rows, :], hot], axis=1)
        part[rows, :] = dot(left, first_table[...]) + edge_bias_ref[...]
        send_hot[rows, :] = onehot_rows(sender_ref[:, rows], send_hot.shape[1])
        ids = lax.broadcasted_iota(jnp.int32, (nodes, tile), 0)
        recv_hot[:, rows] = jnp.where(ids == receiver, 1.0, 0.0).astype(BF16)
        return carry

    pl.semaphore_wait(barrier, patches)

    def to_patch(target):
        return pltpu.make_async_remote_copy(
            src_ref=outgoing.at[target],
            dst_ref=arrived.at[core, me],
            send_sem=send_sem.at[target],
            recv_sem=recv_sem.at[me],
            device_id=(target, core),
            device_id_type=MESH,
        )

    def from_patch(source):
        return pltpu.make_async_remote_copy(
            src_ref=outgoing.at[source],
            dst_ref=arrived.at[core, source],
            send_sem=send_sem.at[source],
            recv_sem=recv_sem.at[source],
            device_id=(source, core),
            device_id_type=MESH,
        )

    def to_core(source, source_ref):
        return pltpu.make_async_remote_copy(
            src_ref=source_ref,
            dst_ref=arrived.at[core, source],
            send_sem=pass_sem.at[source],
            recv_sem=passed_sem.at[source],
            device_id=(me, other),
            device_id_type=MESH,
        )

    def from_core(source):
        return pltpu.make_async_remote_copy(
            src_ref=arrived.at[core, source],
            dst_ref=arrived.at[other, source],
            send_sem=pass_sem.at[source],
            recv_sem=passed_sem.at[source],
            device_id=(me, other),
            device_id_type=MESH,
        )

    def send_step(at, ends):
        target, ends = far_first(at, ends)
        to_patch(target).start()
        return ends

    lax.fori_loop(1, patches, send_step, ends)
    to_core(me, outgoing.at[me]).start()
    arrived[core, me] = outgoing[me]

    loads[2].wait()
    first_table[pl.ds(width, padded), :] = dot(node[...], w_recv[...]).astype(BF16)
    for load in loads[3:7]:
        load.wait()
    lax.fori_loop(0, tiles, first_layer, 0)

    for load in loads[7:]:
        load.wait()
    aggregate[...] = jnp.zeros_like(aggregate)

    def pass_step(step, carry):
        source = lax.rem(me + patches - step, patches)
        from_patch(source).wait_recv()
        to_core(source, arrived.at[core, source]).start()
        return carry

    lax.fori_loop(1, patches, pass_step, 0)

    def passed_step(step, carry):
        from_core(lax.rem(me + patches - step, patches)).wait_recv()
        return carry

    lax.fori_loop(0, patches, passed_step, 0)
    for first in range(0, patches, block):
        rows = jnp.concatenate(
            [arrived[side, first : first + block].reshape(block * slots, half) for side in range(2)],
            axis=1,
        )
        send_table[first * slots : (first + block) * slots, :] = dot(rows, w_send[...]).astype(BF16)

    count = count_ref[0]

    def store(index):
        rows = pl.ds(pl.multiple_of(index * chunk, chunk), chunk)
        return pltpu.make_async_copy(updated.at[rows], new_edge_hbm.at[rows], store_sem.at[index])

    def second_layer(index, carry):
        span = chunk // pieces
        deltas = []
        for piece in range(pieces):
            first = pl.multiple_of(index * chunk, chunk) + piece * span
            rows = pl.ds(first, span)
            pre = part[rows, :] + dot(send_hot[rows, :], send_table[...])
            hidden = silu(pre).astype(BF16)
            message = dot(hidden, edge_out[...]) + edge_out_bias_ref[...]
            delta = layer_norm(message, edge_gain_ref[...], edge_offset_ref[...])
            ids = lax.broadcasted_iota(jnp.int32, (span, width), 0) + first
            delta = jnp.where(ids < count, delta, 0.0).astype(BF16)
            updated[rows, :] = (edges[rows, :].astype(F32) + delta.astype(F32)).astype(BF16)
            deltas.append(delta)
        store(index).start()
        rows = pl.ds(pl.multiple_of(index * chunk, chunk), chunk)
        aggregate[...] += dot(recv_hot[:, rows], jnp.concatenate(deltas, axis=0))
        return carry

    chunks = edge_rows // chunk
    lax.fori_loop(0, chunks, second_layer, 0)

    agg_mine[...] = aggregate[...].astype(BF16)
    exchange = pltpu.make_async_remote_copy(
        src_ref=agg_mine,
        dst_ref=agg_other,
        send_sem=agg_sem.at[0],
        recv_sem=agg_sem.at[1],
        device_id=(me, other),
        device_id_type=MESH,
    )
    exchange.start()

    def sent_step(step, carry):
        source = lax.rem(me + step, patches)
        to_patch(source).wait_send()
        to_core(source, arrived.at[core, source]).wait_send()
        return carry

    lax.fori_loop(1, patches, sent_step, 0)
    to_core(me, outgoing.at[me]).wait_send()

    def stored_step(index, carry):
        store(index).wait()
        return carry

    lax.fori_loop(0, chunks, stored_step, 0)
    exchange.wait()
    summed_ref[...] = (agg_mine[...].astype(F32) + agg_other[...].astype(F32)).astype(BF16)


def node_kernel(
    pieces,
    node_bias_ref,
    node_out_bias_ref,
    node_gain_ref,
    node_offset_ref,
    summed_hbm,
    node_hbm,
    w_node_hbm,
    w_agg_hbm,
    node_out_hbm,
    edge_hbm,
    new_edge_hbm,
    new_node_ref,
    summed,
    node,
    w_node,
    w_agg,
    node_out,
    edges,
    load_sem,
    in_sem,
    out_sem,
):
    rows = edge_hbm.shape[0] // pieces
    loads = [
        pltpu.make_async_copy(source, target, load_sem.at[number])
        for number, (source, target) in enumerate(
            (
                (node_hbm, node),
                (w_node_hbm, w_node),
                (summed_hbm, summed),
                (w_agg_hbm, w_agg),
                (node_out_hbm, node_out),
            )
        )
    ]
    takes = [
        pltpu.make_async_copy(
            edge_hbm.at[pl.ds(at * rows, rows)], edges.at[pl.ds(at * rows, rows)], in_sem.at[at]
        )
        for at in range(pieces)
    ]
    puts = [
        pltpu.make_async_copy(
            edges.at[pl.ds(at * rows, rows)], new_edge_hbm.at[pl.ds(at * rows, rows)], out_sem.at[at]
        )
        for at in range(pieces)
    ]
    for copy in loads + takes:
        copy.start()
    for take, put in zip(takes, puts):
        take.wait()
        put.start()
    for load in loads:
        load.wait()
    node_pre = dot(node[...], w_node[...]) + dot(summed[...], w_agg[...]) + node_bias_ref[...]
    hidden = silu(node_pre).astype(BF16)
    message = dot(hidden, node_out[...]) + node_out_bias_ref[...]
    normed = layer_norm(message, node_gain_ref[...], node_offset_ref[...])
    new_node_ref[...] = (node[...].astype(F32) + normed).astype(BF16)
    for put in puts:
        put.wait()


def on_device(
    patches,
    node_latent,
    edge_latent,
    edge_sender,
    edge_receiver,
    edge_count,
    send_rows,
    w_edge,
    w_send,
    w_recv,
    edge_bias,
    edge_out,
    edge_out_bias,
    edge_gain,
    edge_offset,
    w_node,
    w_agg,
    node_bias,
    node_out,
    node_out_bias,
    node_gain,
    node_offset,
):
    nodes, width = node_latent.shape
    edge_rows = edge_latent.shape[0]
    slots = send_rows.shape[2]
    senders = patches * slots
    padded = round_up(nodes, LANES)
    half = width // 2
    tile = 256
    chunk = 512
    pieces = 1
    tiles = edge_rows // tile
    vmem = pl.BlockSpec(memory_space=pltpu.VMEM)
    smem = pl.BlockSpec(memory_space=pltpu.SMEM)
    hbm = pl.BlockSpec(memory_space=pl.ANY)
    weight = pltpu.VMEM((width, width), BF16)
    vector = pltpu.VMEM((1, width), F32)
    scratch = [
        pltpu.VMEM((patches, slots), jnp.int32),
        pltpu.VMEM((1, edge_rows), jnp.int32),
        pltpu.VMEM((1, edge_rows), jnp.int32),
        vector,
        vector,
        vector,
        vector,
        pltpu.VMEM((padded, width), BF16),
        pltpu.VMEM((edge_rows, width), BF16),
        pltpu.VMEM((width + padded, width), BF16),
        weight,
        weight,
        weight,
        pltpu.VMEM((patches, slots, half), BF16),
        pltpu.VMEM((2, patches, slots, half), BF16),
        pltpu.VMEM((senders, width), BF16),
        pltpu.VMEM((edge_rows, width), F32),
        pltpu.VMEM((edge_rows, senders), BF16),
        pltpu.VMEM((nodes, edge_rows), BF16),
        pltpu.VMEM((edge_rows, width), BF16),
        pltpu.VMEM((nodes, width), F32),
        pltpu.VMEM((nodes, width), BF16),
        pltpu.VMEM((nodes, width), BF16),
    ]
    edge_flops = 2 * edge_rows * width * (2 * width + senders + padded + nodes)
    edge_new, summed = pl.pallas_call(
        functools.partial(edge_kernel, patches, tile, chunk, pieces),
        out_shape=(
            jax.ShapeDtypeStruct(edge_latent.shape, BF16),
            jax.ShapeDtypeStruct(node_latent.shape, BF16),
        ),
        in_specs=[smem] + [hbm] * 13,
        out_specs=(hbm, vmem),
        scratch_shapes=scratch
        + [
            pltpu.SemaphoreType.DMA((12,)),
            pltpu.SemaphoreType.DMA((tiles,)),
            pltpu.SemaphoreType.DMA((edge_rows // chunk,)),
            pltpu.SemaphoreType.DMA((patches,)),
            pltpu.SemaphoreType.DMA((patches,)),
            pltpu.SemaphoreType.DMA((patches,)),
            pltpu.SemaphoreType.DMA((patches,)),
            pltpu.SemaphoreType.DMA((2,)),
        ],
        cost_estimate=pl.CostEstimate(
            flops=edge_flops, bytes_accessed=4 * edge_rows * width, transcendentals=0
        ),
        compiler_params=pltpu.CompilerParams(
            collective_id=0, has_side_effects=True, vmem_limit_bytes=62 * 1024 * 1024
        ),
    )(
        edge_count,
        send_rows.reshape(patches, slots),
        edge_sender.reshape(1, edge_rows),
        edge_receiver.reshape(1, edge_rows),
        edge_bias.reshape(1, width),
        edge_out_bias.reshape(1, width),
        edge_gain.reshape(1, width),
        edge_offset.reshape(1, width),
        node_latent,
        edge_latent,
        w_edge,
        w_send,
        w_recv,
        edge_out,
    )
    node_pieces = 4
    rows = pltpu.VMEM((nodes, width), BF16)
    return pl.pallas_call(
        functools.partial(node_kernel, node_pieces),
        out_shape=(
            jax.ShapeDtypeStruct(edge_latent.shape, BF16),
            jax.ShapeDtypeStruct(node_latent.shape, BF16),
        ),
        in_specs=[vmem] * 4 + [hbm] * 6,
        out_specs=(hbm, vmem),
        scratch_shapes=[
            rows,
            rows,
            weight,
            weight,
            weight,
            pltpu.VMEM((edge_rows, width), BF16),
            pltpu.SemaphoreType.DMA((5,)),
            pltpu.SemaphoreType.DMA((node_pieces,)),
            pltpu.SemaphoreType.DMA((node_pieces,)),
        ],
        compiler_params=pltpu.CompilerParams(vmem_limit_bytes=60 * 1024 * 1024),
    )(
        node_bias.reshape(1, width),
        node_out_bias.reshape(1, width),
        node_gain.reshape(1, width),
        node_offset.reshape(1, width),
        summed,
        node_latent,
        w_node,
        w_agg,
        node_out,
        edge_new,
    )


def solution(mesh):
    placed = (
        P("patch", None),
        P(("patch", "pair"), None),
        P(("patch", "pair")),
        P(("patch", "pair")),
        P(("patch", "pair")),
        P("patch", None, None),
    ) + (P(),) * 15
    return jax.shard_map(
        functools.partial(on_device, mesh.shape["patch"]),
        mesh=mesh,
        in_specs=placed,
        out_specs=(P(("patch", "pair"), None), P("patch", None)),
        check_vma=False,
    )
```
